32 devices in a mesh: vocab: 8 (over y, x, core), dp: 4 (over z).
Axes of the slice: x: 2, y: 2, z: 4, core: 2. Of those that a mesh axis runs over, the one named last changes fastest.
Arguments:
- token_ids: int32 [8192], P(('vocab', 'dp')), may hold values from 0 to 50256
- target_ids: int32 [8192], P(('vocab', 'dp')), may hold values from 0 to 50256
- loss_mask: int32 [8192], P(('vocab', 'dp')), may hold values from 0 to 1, as said below
- seq_ids: int32 [8192], P(('vocab', 'dp')), may hold values from 0 to 255, as said below
- embed_table: bfloat16 [50304, 1024], P('vocab'), may hold values from -0.359375 to 0.359375
- pos_table: bfloat16 [1024, 1024], replicated, may hold values from -0.359375 to 0.359375
- gains: float32 [3, 1024], replicated, may hold values from 0.5 to 1.5
- shifts: float32 [3, 1024], replicated, may hold values from -1.8 to 1.8
- linear_bias: float32 [1, 9216], replicated, may hold values from -1.8 to 1.8
- query_key_value_weight: bfloat16 [1, 1024, 3072], replicated, may hold values from -0.1875 to 0.1875
- w_out: bfloat16 [1, 1024, 1024], replicated, may hold values from -0.5 to 0.5
- w_fc: bfloat16 [1, 1024, 4096], replicated, may hold values from -0.1875 to 0.1875
- w_proj: bfloat16 [1, 4096, 1024], replicated, may hold values from -0.09375 to 0.09375
- adapters: float32 [1, 24576], P(None, 'vocab'), may hold values from -0.18 to 0.18
- first_moment: float32 [1, 24576], P(None, 'vocab'), may hold values from -4.2483338e-05 to 4.2483338e-05
- second_moment: float32 [1, 24576], P(None, 'vocab'), may hold values from 2.0345052e-12 to 3.2552083e-11
- step_count: int32 [1], replicated, may hold values from 2 to 20
Outputs:
- loss: float32 [], replicated
- grad_norm: float32 [], replicated
- new_adapters: float32 [1, 24576], P(None, 'vocab')
- new_first: float32 [1, 24576], P(None, 'vocab')
- new_second: float32 [1, 24576], P(None, 'vocab')
- adapter_copy: bfloat16 [1, 24576], P(None, 'vocab')
The draws below stay inside these ranges and needn't reach their ends.
Inputs may be any that keep to these rules, and one draw needn't show every extreme that they name: seq_ids never falls; the tokens of each device form whole sequences of 256 // 8 times 1, 2, 4 or 8 tokens, each starting at a multiple of its length within the device; some device holds one sequence of 256 tokens and some device eight of 32. `token_ids`: every id is a real row, below 50257. `target_ids`: every target is a real row, below 50257. `loss_mask`: the share of ones differs from device to device; some devices have all ones.
All inputs are finite; a program needn't handle non-finite values.
Results may differ from the reference program's by a relative error of at most 0.0051.
Values may be sent and summed in bfloat16 or wider, within the bound.
A program may use at most 256 MiB of HBM per device.

```python
import math
import jax
import jax.numpy as jnp
import numpy as np
from jax import lax

MODEL_WIDTH = 1024
HEADS = 16
HEAD_DIM = 64
FF = 4096
VOCAB = 50304
VOCAB_REAL = 50257
CTX = 1024
RANK = 4
LAYERS = 1
TOK_DEV = 256
TOKENS = 8192
ADAPT = 24576
N_DP = 4


def draw_seq_ids(key, part):
    dev_count = TOKENS // TOK_DEV
    split_bits = jax.random.randint(key, (dev_count, 7), 0, 2)
    device_col = jnp.arange(dev_count)[:, None]
    column = jnp.arange(7)[None, :]
    split_bits = jnp.where((device_col == 0) & (column == 0), 0, split_bits)
    split_bits = jnp.where(device_col == dev_count - 1, 1, split_bits)
    whole_cut = split_bits[:, 0]
    left_half = whole_cut * split_bits[:, 1]
    right_half = whole_cut * split_bits[:, 2]
    boundary = jnp.stack([jnp.zeros_like(whole_cut), left_half * split_bits[:, 3], left_half, left_half * split_bits[:, 4], whole_cut, right_half * split_bits[:, 5], right_half, right_half * split_bits[:, 6]], axis=1)
    local_ids = jnp.cumsum(boundary, axis=1)
    unit_ids = local_ids + 8 * device_col
    return jnp.repeat(unit_ids, TOK_DEV // 8, axis=1).reshape(TOKENS).astype(jnp.int32)


def draw_loss_mask(key, part):
    dev_count = TOKENS // TOK_DEV
    ranking = jax.random.permutation(jax.random.fold_in(key, 11), N_DP)
    device_rank = ranking[jnp.arange(dev_count) % N_DP]
    rolls = jax.random.randint(jax.random.fold_in(key, 12), (dev_count, TOK_DEV), 0, N_DP)
    kept = (rolls <= device_rank[:, None]).astype(jnp.int32)
    return kept.reshape(TOKENS)


def place_ends(entries, key, smallest, top_value):
    longest = entries.shape.index(max(entries.shape))
    spots = []
    for shift in (0, 1):
        where = [jax.random.randint(jax.random.fold_in(key, axis), (), 0, length) for axis, length in enumerate(entries.shape)]
        where[longest] = (where[longest] + shift) % entries.shape[longest]
        spots.append(tuple(where))
    return entries.at[spots[0]].set(smallest).at[spots[1]].set(top_value)


def block_scale(stream_key, dims, cuts, smallest, top_value):
    factor_of, own = 1.0, jax.random.fold_in(stream_key, 6)
    for position, blocks in cuts:
        draws = jnp.exp(jax.random.uniform(jax.random.fold_in(own, position), (blocks,), jnp.float32, smallest / len(cuts), top_value / len(cuts)))
        factor_of = factor_of * jnp.repeat(draws, dims[position] // blocks).reshape([-1 if axis == position else 1 for axis in range(len(dims))])
    return factor_of


def rank_bounds(number_of, skew):
    portions = [(1 << 20) // math.isqrt(standing ** skew) + 1 for standing in range(1, number_of + 1)]
    deviation = 1 + sum(portions) // (1 << 30)
    return np.cumsum(np.array([max(1, weight // deviation) for weight in portions]))


def ranked_ids(key, dims, amount, slope):
    grid = rank_bounds(amount, slope)
    pick = jax.random.randint(jax.random.fold_in(key, 1), dims, 0, int(grid[amount - 1]))
    grade = jnp.searchsorted(jnp.asarray(grid, jnp.int32), pick, side="right")
    return jax.random.permutation(jax.random.fold_in(key, 2), amount)[grade].astype(jnp.int32)


def scatter_about(rng, dims, scale, limit, shards=(), kind=jnp.bfloat16):
    drawn = jax.random.normal(rng, dims, jnp.float32) * scale
    if len(shards) > 0:
        drawn = block_scale(rng, dims, shards, -0.22, 0.18) * drawn
    return jnp.clip(drawn, min=-limit, max=limit).astype(kind)


def setup_inputs(seed: int = 0) -> dict:
    key_list = jax.random.split(jax.random.key(seed), 18)
    return {
        "token_ids": place_ends(ranked_ids(key_list[0], (TOKENS,), VOCAB_REAL, 2), jax.random.fold_in(key_list[0], 3), 0, VOCAB_REAL - 1).astype(jnp.int32),
        "target_ids": place_ends(jax.random.randint(key_list[1], (TOKENS,), 0, VOCAB_REAL), jax.random.fold_in(key_list[1], 1), 0, VOCAB_REAL - 1).astype(jnp.int32),
        "loss_mask": draw_loss_mask(jax.random.fold_in(key_list[17], 71), 0),
        "seq_ids": draw_seq_ids(jax.random.fold_in(key_list[17], 71), 0),
        "embed_table": scatter_about(key_list[4], (VOCAB, MODEL_WIDTH), 0.06, 0.359375, ((0, 8),)),
        "pos_table": scatter_about(key_list[5], (CTX, MODEL_WIDTH), 0.06, 0.359375),
        "gains": jnp.clip(1.0 + 0.1 * jax.random.normal(key_list[6], (2 * LAYERS + 1, MODEL_WIDTH), jnp.float32), 0.5, 1.5),
        "shifts": scatter_about(key_list[7], (2 * LAYERS + 1, MODEL_WIDTH), 0.3, 1.8, (), jnp.float32),
        "linear_bias": scatter_about(key_list[8], (LAYERS, 5 * MODEL_WIDTH + FF), 0.3, 1.8, (), jnp.float32),
        "query_key_value_weight": scatter_about(key_list[9], (LAYERS, MODEL_WIDTH, 3 * MODEL_WIDTH), MODEL_WIDTH ** -0.5, 0.1875),
        "w_out": scatter_about(key_list[10], (LAYERS, MODEL_WIDTH, MODEL_WIDTH), (MODEL_WIDTH // 8) ** -0.5, 0.5),
        "w_fc": scatter_about(key_list[11], (LAYERS, MODEL_WIDTH, FF), MODEL_WIDTH ** -0.5, 0.1875),
        "w_proj": scatter_about(key_list[12], (LAYERS, FF, MODEL_WIDTH), FF ** -0.5, 0.09375),
        "adapters": scatter_about(key_list[13], (LAYERS, ADAPT), 0.03, 0.18, ((1, 8),), jnp.float32),
        "first_moment": scatter_about(key_list[14], (LAYERS, ADAPT), (0.111 * 0.01 / (LAYERS * ADAPT) ** 0.5), 4.2483337892917916e-05, ((1, 8),), jnp.float32),
        "second_moment": jnp.clip(jnp.exp(math.log(3.255208255725783e-11) - 2.7725887 * jax.random.uniform(key_list[15], (LAYERS, ADAPT), jnp.float32) ** block_scale(key_list[15], (LAYERS, ADAPT), ((1, 8),), -0.2, 0.2)), 2.0345051598286146e-12, 3.255208255725783e-11),
        "step_count": jax.random.randint(key_list[16], (1,), 2, 21).astype(jnp.int32),
    }


PRECISE = lax.Precision.HIGHEST
ADAPTER_SCALE = 8.0
CLIP_NORM = 0.01
BETA_ONE = 0.9
BETA_TWO = 0.999
ADAM_EPS = 1e-08
WEIGHT_DECAY = 0.01
LEARN_RATE = 0.02

@jax.custom_vjp
def low(v):
    return lax.optimization_barrier(v.astype(jnp.bfloat16)).astype(jnp.float32)

@jax.custom_vjp
def low_back(v):
    return v

def low_keep(v):
    return (low(v), None)

def low_pass(kept, grad):
    return (grad,)

def back_keep(v):
    return (v, None)

def back_low(kept, grad):
    return (low(grad),)
low.defvjp(low_keep, low_pass)
low_back.defvjp(back_keep, back_low)

def matrix_product(left, right):
    return jnp.dot(left, right, precision=PRECISE)

def layer_norm(values, gain, shift):
    center = values - lax.optimization_barrier(jnp.mean(values, -1, keepdims=True))
    spread = lax.optimization_barrier(jnp.mean(center * center, -1, keepdims=True))
    return center * lax.rsqrt(spread + 1e-05) * gain + shift

def gelu(values):
    return 0.5 * values * (1.0 + jnp.tanh(0.7978845608028654 * (values + 0.044715 * values * values * values)))

def positions_of(seq):
    place = jnp.arange(seq.shape[0], dtype=jnp.int32)
    fresh = jnp.concatenate([jnp.ones((1,), bool), seq[1:] != seq[:-1]])
    start = lax.cummax(jnp.where(fresh, place, 0).astype(jnp.int32))
    return place - start

def split_adapter(flat):
    width = MODEL_WIDTH * RANK
    qkv_down_matrix = flat[:width].reshape(MODEL_WIDTH, RANK)
    output_down_matrix = flat[width:2 * width].reshape(MODEL_WIDTH, RANK)
    qkv_up_matrix = flat[2 * width:5 * width].reshape(RANK, 3 * MODEL_WIDTH)
    output_up_matrix = flat[5 * width:].reshape(RANK, MODEL_WIDTH)
    return (qkv_down_matrix, output_down_matrix, qkv_up_matrix, output_up_matrix)

def attend(query_key_value, seq):
    block_rows = 4 * TOK_DEV
    blocks = query_key_value.shape[0] // block_rows

    def one_block(pair):
        part, seq_block = pair
        query = part[:, :MODEL_WIDTH].reshape(block_rows, HEADS, HEAD_DIM)
        keys = part[:, MODEL_WIDTH:2 * MODEL_WIDTH].reshape(block_rows, HEADS, HEAD_DIM)
        values = part[:, 2 * MODEL_WIDTH:].reshape(block_rows, HEADS, HEAD_DIM)
        scores = low_back(jnp.einsum('qhd,khd->hqk', query, keys, precision=PRECISE) * 0.125)
        place = jnp.arange(block_rows)
        visible = (seq_block[:, None] == seq_block[None, :]) & (place[None, :] <= place[:, None])
        scores = jnp.where(visible[None], scores, -1e+30)
        probs = low(jax.nn.softmax(scores, axis=-1))
        return jnp.einsum('hqk,khd->qhd', probs, values, precision=PRECISE).reshape(block_rows, MODEL_WIDTH)
    outs = lax.map(jax.checkpoint(one_block), (query_key_value.reshape(blocks, block_rows, 3 * MODEL_WIDTH), seq.reshape(blocks, block_rows)))
    return outs.reshape(-1, MODEL_WIDTH)

def reference(token_ids, target_ids, loss_mask, seq_ids, embed_table, pos_table, gains, shifts, linear_bias, query_key_value_weight, w_out, w_fc, w_proj, adapters, first_moment, second_moment, step_count):
    table = embed_table.astype(jnp.float32)
    pos_rows = pos_table.astype(jnp.float32)
    query_key_value_stack = query_key_value_weight.astype(jnp.float32)
    output_weight_stack = w_out.astype(jnp.float32)
    wf_all = w_fc.astype(jnp.float32)
    wp_all = w_proj.astype(jnp.float32)
    positions = positions_of(seq_ids)
    live = jnp.arange(VOCAB) < VOCAB_REAL
    weights = loss_mask.astype(jnp.float32)

    def loss_of(master):
        rounded = low(master)
        resid = table[token_ids] + pos_rows[positions]
        for layer_params in range(LAYERS):
            qkv_down_matrix, output_down_matrix, qkv_up_matrix, output_up_matrix = split_adapter(rounded[layer_params])
            bias_vector = linear_bias[layer_params]
            hidden_first = low(layer_norm(resid, gains[2 * layer_params], shifts[2 * layer_params]))
            adapter_input = low(matrix_product(hidden_first, qkv_down_matrix))
            query_key_value = matrix_product(hidden_first, query_key_value_stack[layer_params]) + bias_vector[:3 * MODEL_WIDTH] + ADAPTER_SCALE * matrix_product(adapter_input, qkv_up_matrix)
            query_key_value = low(low_back(query_key_value))
            attention_output = low(low_back(attend(query_key_value, seq_ids)))
            adapter_middle = low(matrix_product(attention_output, output_down_matrix))
            adapter_branch = matrix_product(attention_output, output_weight_stack[layer_params]) + bias_vector[3 * MODEL_WIDTH:4 * MODEL_WIDTH] + ADAPTER_SCALE * matrix_product(adapter_middle, output_up_matrix)
            resid = resid + low_back(adapter_branch)
            h_two = low(layer_norm(resid, gains[2 * layer_params + 1], shifts[2 * layer_params + 1]))
            pre = low_back(matrix_product(h_two, wf_all[layer_params]) + bias_vector[4 * MODEL_WIDTH:4 * MODEL_WIDTH + FF])
            act = low(gelu(pre))
            resid = resid + low_back(matrix_product(act, wp_all[layer_params]) + bias_vector[4 * MODEL_WIDTH + FF:])
        hidden = low(layer_norm(resid, gains[2 * LAYERS], shifts[2 * LAYERS]))

        def head(triple):
            row_block, target_block, weight_block = triple
            logits = low_back(matrix_product(row_block, table.T))
            logits = jnp.where(live[None], logits, -1e+30)
            row_lse = jax.nn.logsumexp(logits, axis=-1)
            picked = jnp.take_along_axis(logits, target_block[:, None], axis=1)[:, 0]
            return jnp.sum(weight_block * (row_lse - picked))
        sums = lax.map(jax.checkpoint(head), (hidden.reshape(-1, 512, MODEL_WIDTH), target_ids.reshape(-1, 512), weights.reshape(-1, 512)))
        return jnp.sum(sums) / TOKENS
    loss, pull = jax.vjp(loss_of, adapters)
    grad = pull(jnp.ones((), jnp.float32))[0]
    grad_norm = jnp.sqrt(jnp.sum(grad * grad))
    clipped = grad * jnp.minimum(1.0, CLIP_NORM / (grad_norm + 1e-06))
    step = step_count[0].astype(jnp.float32)
    new_first = BETA_ONE * first_moment + (1.0 - BETA_ONE) * clipped
    new_second = BETA_TWO * second_moment + (1.0 - BETA_TWO) * clipped * clipped
    fix_one = 1.0 - jnp.power(BETA_ONE, step)
    fix_two = 1.0 - jnp.power(BETA_TWO, step)
    motion = new_first / fix_one / (jnp.sqrt(new_second / fix_two) + ADAM_EPS) + WEIGHT_DECAY * adapters
    new_adapters = adapters - LEARN_RATE * motion
    return (loss, grad_norm, new_adapters, new_first, new_second, new_adapters.astype(jnp.bfloat16))
```

```python
import functools
import math

import jax
import jax.numpy as jnp
from jax import lax
from jax.experimental import pallas as pl
from jax.experimental.pallas import tpu as pltpu
from jax.sharding import PartitionSpec as P

MODEL_WIDTH = 1024
HEADS = 16
HEAD_DIM = 64
FF = 4096
VOCAB_REAL = 50257
RANK = 4
LAYERS = 1
TOK_DEV = 256


PRECISE = lax.Precision.HIGHEST
ADAPTER_SCALE = 8.0
CLIP_NORM = 0.01
BETA_ONE = 0.9
BETA_TWO = 0.999
ADAM_EPS = 1e-08
WEIGHT_DECAY = 0.01
LEARN_RATE = 0.02


def mixed_product(left, right):
    return jnp.dot(left, right, preferred_element_type=jnp.float32)


def exact_product(left, right):
    return jnp.dot(left.astype(jnp.float32), right.astype(jnp.float32), precision=PRECISE)


def layer_norm(values, gain, shift):
    center = values - jnp.mean(values, -1, keepdims=True)
    spread = jnp.mean(center * center, -1, keepdims=True)
    inverse = lax.rsqrt(spread + 1e-05)
    normed = center * inverse
    return (normed * gain + shift, normed, inverse)


def norm_back(grad_in, normed, inverse, gain):
    scaled = grad_in * gain
    return inverse * (
        scaled
        - jnp.mean(scaled, -1, keepdims=True)
        - normed * jnp.mean(scaled * normed, -1, keepdims=True)
    )


def gelu(values):
    return (
        0.5
        * values
        * (1.0 + jnp.tanh(0.7978845608028654 * (values + 0.044715 * values * values * values)))
    )


def positions_of(seq):
    place = jnp.arange(seq.shape[0], dtype=jnp.int32)
    fresh = jnp.concatenate([jnp.ones((1,), bool), seq[1:] != seq[:-1]])
    start = lax.cummax(jnp.where(fresh, place, 0))
    return place - start


def split_adapter(flat):
    width = MODEL_WIDTH * RANK
    qkv_down_matrix = flat[:width].reshape(MODEL_WIDTH, RANK)
    output_down_matrix = flat[width : 2 * width].reshape(MODEL_WIDTH, RANK)
    qkv_up_matrix = flat[2 * width : 5 * width].reshape(RANK, 3 * MODEL_WIDTH)
    output_up_matrix = flat[5 * width :].reshape(RANK, MODEL_WIDTH)
    return (qkv_down_matrix, output_down_matrix, qkv_up_matrix, output_up_matrix)


def split_heads(query_key_value):
    count = query_key_value.shape[0]
    query = query_key_value[:, :MODEL_WIDTH].reshape(count, HEADS, HEAD_DIM)
    keys = query_key_value[:, MODEL_WIDTH : 2 * MODEL_WIDTH].reshape(count, HEADS, HEAD_DIM)
    values = query_key_value[:, 2 * MODEL_WIDTH :].reshape(count, HEADS, HEAD_DIM)
    return (query, keys, values)


def attention_forward(query_key_value, visible):
    query, keys, values = split_heads(query_key_value)
    scores = jnp.einsum("qhd,khd->hqk", query, keys, preferred_element_type=jnp.float32) * 0.125
    scores = jnp.where(visible[None], scores, -1e30)
    row_top = jnp.max(scores, -1, keepdims=True)
    expd = jnp.exp(scores - row_top)
    row_total = jnp.sum(expd, -1, keepdims=True)
    probs = (expd / row_total).astype(jnp.bfloat16)
    attention_output = jnp.einsum("hqk,khd->qhd", probs, values, preferred_element_type=jnp.float32)
    return (
        attention_output.reshape(query_key_value.shape[0], MODEL_WIDTH),
        row_top + jnp.log(row_total),
    )


def attention_back(query_key_value, visible, row_lse, attention_output_gradient):
    query, keys, values = split_heads(query_key_value)
    count = query_key_value.shape[0]
    scores = jnp.einsum("qhd,khd->hqk", query, keys, preferred_element_type=jnp.float32) * 0.125
    probs = jnp.where(visible[None], jnp.exp(scores - row_lse), 0.0)
    grad_heads = attention_output_gradient.reshape(count, HEADS, HEAD_DIM)
    grad_probs = jnp.einsum("qhd,khd->hqk", grad_heads, values, preferred_element_type=jnp.float32)
    grad_values = jnp.einsum(
        "hqk,qhd->khd", probs.astype(jnp.bfloat16), grad_heads, preferred_element_type=jnp.float32
    )
    grad_scores = probs * (grad_probs - jnp.sum(probs * grad_probs, -1, keepdims=True))
    grad_scores = grad_scores.astype(jnp.bfloat16)
    grad_query = (
        jnp.einsum("hqk,khd->qhd", grad_scores, keys, preferred_element_type=jnp.float32) * 0.125
    )
    grad_keys = (
        jnp.einsum("hqk,qhd->khd", grad_scores, query, preferred_element_type=jnp.float32) * 0.125
    )
    joined = jnp.concatenate(
        [
            grad_query.reshape(count, MODEL_WIDTH),
            grad_keys.reshape(count, MODEL_WIDTH),
            grad_values.reshape(count, MODEL_WIDTH),
        ],
        axis=1,
    )
    return joined.astype(jnp.bfloat16)


MESH = pl.DeviceIdType.MESH
VMEM_CAP = 66 * 1000 * 1000
NEG = -1e30


def vspec():
    return pl.BlockSpec(memory_space=pltpu.VMEM)


def aspec():
    return pl.BlockSpec(memory_space=pl.ANY)


def xor_of(left, right, count):
    total, bit = 0, 1
    while bit < count:
        total = total + ((left // bit + right // bit) % 2) * bit
        bit *= 2
    return total


def greet(axis_counts):
    barrier = pltpu.get_barrier_semaphore()
    waits = 0
    for axis, count in axis_counts:
        me = lax.axis_index(axis)
        for step in range(1, count):
            pl.semaphore_signal(
                barrier, inc=1, device_id={axis: lax.rem(me + step, count)}, device_id_type=MESH
            )
        waits += count - 1
    pl.semaphore_wait(barrier, waits)


def push(src, dst, send_sem, recv_sem, axis, peer):
    return pltpu.make_async_remote_copy(
        src_ref=src,
        dst_ref=dst,
        send_sem=send_sem,
        recv_sem=recv_sem,
        device_id={axis: peer},
        device_id_type=MESH,
    )


def meta_kernel(n, ints_ref, adapt_ref, all_ints, all_adapt, send_sem, recv_sem):
    me = lax.axis_index("vocab")
    greet((("vocab", n),))
    copies = []
    for step in range(1, n):
        peer = lax.rem(me + step, n)
        for kind, (src, dst) in enumerate(((ints_ref, all_ints), (adapt_ref, all_adapt))):
            copy = push(
                src,
                dst.at[me],
                send_sem.at[kind, step],
                recv_sem.at[kind, step],
                "vocab",
                peer,
            )
            copy.start()
            copies.append(copy)
    all_ints[me] = ints_ref[...]
    all_adapt[me] = adapt_ref[...]
    for copy in copies:
        copy.wait()


def gather_meta(n, ints, adapt):
    return pl.pallas_call(
        functools.partial(meta_kernel, n),
        out_shape=(
            jax.ShapeDtypeStruct((n,) + ints.shape, ints.dtype),
            jax.ShapeDtypeStruct((n,) + adapt.shape, adapt.dtype),
        ),
        in_specs=[vspec(), vspec()],
        out_specs=(vspec(), vspec()),
        scratch_shapes=[pltpu.SemaphoreType.DMA((2, n)), pltpu.SemaphoreType.DMA((2, n))],
        compiler_params=pltpu.CompilerParams(collective_id=1, has_side_effects=True),
        name="gather_meta",
    )(ints, adapt)


def finish_kernel(
    n, z, rows, total_tokens,
    grads, adapt_ref, first_ref, second_ref, step_ref,
    loss_out, norm_out, adapt_out, first_out, second_out, copy_out,
    got_one, got_two, got_three, shard, squares, send_one, recv_one, send_two, recv_two, send_three, recv_three,
):
    me, mz = lax.axis_index("vocab"), lax.axis_index("dp")
    greet((("vocab", n), ("dp", z)))
    copies = []
    for step in range(1, n):
        peer = lax.rem(me + step, n)
        copy = push(grads.at[peer], got_one.at[me], send_one.at[step], recv_one.at[step], "vocab", peer)
        copy.start()
        copies.append(copy)
    got_one[me] = grads[me]
    for copy in copies:
        copy.wait()
    total = got_one[0]
    for source in range(1, n):
        total = total + got_one[source]
    shard[...] = total
    copies = []
    for step in range(1, z):
        peer = lax.rem(mz + step, z)
        copy = push(shard, got_two.at[mz], send_two.at[step], recv_two.at[step], "dp", peer)
        copy.start()
        copies.append(copy)
    got_two[mz] = total
    for copy in copies:
        copy.wait()
    total = got_two[0]
    for source in range(1, z):
        total = total + got_two[source]
    shard[...] = total
    grad = shard[:rows]
    lanes = jnp.sum(grad * grad, axis=0, keepdims=True)
    part = jnp.broadcast_to(lanes, squares.shape)
    squares[...] = part
    copies = []
    for step in range(1, n):
        peer = lax.rem(me + step, n)
        copy = push(squares, got_three.at[me], send_three.at[step], recv_three.at[step], "vocab", peer)
        copy.start()
        copies.append(copy)
    got_three[me] = part
    for copy in copies:
        copy.wait()
    lanes = got_three[0]
    for source in range(1, n):
        lanes = lanes + got_three[source]
    square_sum = jnp.sum(lanes[:1], axis=1, keepdims=True)
    norm = jnp.sqrt(square_sum)
    loss = jnp.sum(shard[rows : rows + 1], axis=1, keepdims=True) * (1.0 / total_tokens)
    loss_out[...] = jnp.broadcast_to(loss, loss_out.shape)
    norm_out[...] = jnp.broadcast_to(norm, norm_out.shape)
    clipped = grad * jnp.minimum(1.0, CLIP_NORM / (norm + 1e-06))
    count = jnp.full((1, 128), step_ref[0], jnp.int32).astype(jnp.float32)
    fix_one = 1.0 - jnp.exp(count * math.log(BETA_ONE))
    fix_two = 1.0 - jnp.exp(count * math.log(BETA_TWO))
    new_first = BETA_ONE * first_ref[...] + (1.0 - BETA_ONE) * clipped
    new_second = BETA_TWO * second_ref[...] + (1.0 - BETA_TWO) * clipped * clipped
    master = adapt_ref[...]
    motion = (
        new_first / fix_one / (jnp.sqrt(new_second / fix_two) + ADAM_EPS) + WEIGHT_DECAY * master
    )
    new_master = master - LEARN_RATE * motion
    adapt_out[...] = new_master
    first_out[...] = new_first
    second_out[...] = new_second
    copy_out[...] = new_master.astype(jnp.bfloat16)


def finish(n, z, total_tokens, grads, adapters, first, second, step):
    rows, block = adapters.shape[0], grads.shape[1]
    f32 = jnp.float32
    flat = jax.ShapeDtypeStruct((rows, 128), f32)
    tile = jax.ShapeDtypeStruct((8, 128), f32)
    dma = pltpu.SemaphoreType.DMA
    return pl.pallas_call(
        functools.partial(finish_kernel, n, z, rows, total_tokens),
        out_shape=(tile, tile, flat, flat, flat, jax.ShapeDtypeStruct((rows, 128), jnp.bfloat16)),
        in_specs=[vspec()] * 4 + [pl.BlockSpec(memory_space=pltpu.SMEM)],
        out_specs=(vspec(),) * 6,
        scratch_shapes=[
            pltpu.VMEM((n, block, 128), f32),
            pltpu.VMEM((z, block, 128), f32),
            pltpu.VMEM((n, 8, 128), f32),
            pltpu.VMEM((block, 128), f32),
            pltpu.VMEM((8, 128), f32),
            dma((n,)), dma((n,)), dma((z,)), dma((z,)), dma((n,)), dma((n,)),
        ],
        compiler_params=pltpu.CompilerParams(collective_id=2, has_side_effects=True),
        name="finish",
    )(grads, adapters, first, second, step)


def head_kernel(
    n, rows, padded, chunk, vocab_real,
    hid_ref, targets_ref, weights_ref, table_ref,
    dhid_out, loss_out,
    table, probs, hid_all, logit_a, logit_b, tops, run_top, run_sum, run_pick, columns,
    stats, got_stats, lse_cols, dl_a, dl_b, partial, sib_send, off_send,
    load_sem, own_sem, hid_send, hid_recv, fwd_send, stat_send, stat_recv, sib_sem, sib_recv, off_sem, off_recv,
):
    f32, bf16 = jnp.float32, jnp.bfloat16
    tokens, width = hid_ref.shape
    pairs, chunks, ring = n // 2, padded // chunk, off_send.shape[0]
    me = lax.axis_index("vocab")
    sibling = xor_of(me, 1, n)
    held = table_ref.shape[0]
    load = pltpu.make_async_copy(table_ref, table.at[pl.ds(0, held)], load_sem)
    load.start()
    own = pltpu.make_async_copy(hid_ref, hid_all.at[0], own_sem)
    own.start()
    if padded > held:
        table[held:] = jnp.zeros((padded - held, width), bf16)
    greet((("vocab", n),))

    for slot in (1,) + tuple(range(2, n, 2)):
        push(hid_ref, hid_all.at[slot], hid_send.at[slot], hid_recv.at[slot], "vocab", xor_of(me, slot, n)).start()

    lane = lax.broadcasted_iota(jnp.int32, (tokens, 128), 1)
    flane = lane.astype(f32)
    step_rows = 32
    small_lane = lax.broadcasted_iota(jnp.int32, (step_rows, 128), 1).astype(f32)

    base = (me * rows).astype(f32)
    pad_rows = 128 - n
    goals = targets_ref[...] - base
    goals = jnp.where(jnp.logical_and(goals >= 0.0, goals < float(rows)), goals, -1.0)
    columns[...] = jnp.concatenate([goals, jnp.zeros((pad_rows, tokens), f32)], axis=0).T

    def column_of(array, index):
        return jnp.sum(jnp.where(lane == index, array, 0.0), axis=1, keepdims=True)

    stats[...] = jnp.zeros(stats.shape, f32)
    live = jnp.minimum(rows, vocab_real - me * rows).astype(f32)
    dead_from = rows - (rows * n - vocab_real)

    def soft_chunk(slot, index, logit, target):
        for first in range(0, tokens, step_rows):
            part = slice(first, first + step_rows)
            old = run_top[part]
            top = old
            ragged = (index + 1) * chunk > dead_from
            for q in range(0, chunk, 128):
                if ragged and index * chunk + q + 128 > dead_from:
                    kept = jnp.where(small_lane + float(index * chunk + q) < live, logit[part, q : q + 128], NEG)
                    logit[part, q : q + 128] = kept
                    top = jnp.maximum(top, kept)
                else:
                    top = jnp.maximum(top, logit[part, q : q + 128])
            total = run_sum[part] * jnp.exp(old - top)
            pick = run_pick[part]
            goal = target[part]
            for q in range(0, chunk, 128):
                value = logit[part, q : q + 128]
                grown = jnp.exp(value - top)
                total = total + grown
                pick = jnp.where(small_lane + float(index * chunk + q) == goal, value, pick)
                probs[slot, part, index * chunk + q : index * chunk + q + 128] = grown.astype(bf16)
            tops[slot, index, part] = top
            run_top[part] = top
            run_sum[part] = total
            run_pick[part] = pick

    def first_pass(slot, _):
        even = lax.rem(slot, 2) == 0

        @pl.when(slot > 0)
        def _():
            push(hid_ref, hid_all.at[slot], hid_send.at[slot], hid_recv.at[slot], "vocab", sibling).wait_recv()

        @pl.when(jnp.logical_and(slot > 0, even))
        def _():
            push(
                hid_all.at[slot], hid_all.at[slot + 1], fwd_send.at[slot], hid_recv.at[slot + 1], "vocab", sibling
            ).start()

        block = xor_of(me, slot, n)
        target = jnp.broadcast_to(column_of(columns[...], block), (tokens, 128))
        run_top[...] = jnp.full((tokens, 128), NEG, f32)
        run_sum[...] = jnp.zeros((tokens, 128), f32)
        run_pick[...] = jnp.zeros((tokens, 128), f32)
        logit = (logit_a, logit_b)
        for index in range(chunks):
            logit[index % 2][...] = lax.dot_general(
                hid_all[slot],
                table[index * chunk : (index + 1) * chunk],
                (((1,), (1,)), ((), ())),
                preferred_element_type=f32,
            )
            if index > 0:
                soft_chunk(slot, index - 1, logit[(index - 1) % 2], target)
        soft_chunk(slot, chunks - 1, logit[(chunks - 1) % 2], target)
        lane_top = run_top[...]
        top = jnp.max(lane_top, axis=1, keepdims=True)
        total = jnp.sum(run_sum[...] * jnp.exp(lane_top - top), axis=1, keepdims=True)
        pick = jnp.sum(run_pick[...], axis=1, keepdims=True)
        stats[...] = jnp.where(
            lane == block,
            top,
            jnp.where(lane == block + n, total, jnp.where(lane == block + 2 * n, pick, stats[...])),
        )
        return 0

    own.wait()
    load.wait()
    lax.fori_loop(0, n, first_pass, 0)

    for slot in (1,) + tuple(range(2, n, 2)):
        push(hid_ref, hid_all.at[slot], hid_send.at[slot], hid_recv.at[slot], "vocab", sibling).wait_send()
    for slot in range(2, n, 2):
        push(hid_all.at[slot], hid_all.at[slot + 1], fwd_send.at[slot], hid_recv.at[slot + 1], "vocab", sibling).wait_send()

    got_stats[0] = stats[...].T[: 3 * n]
    copies = []
    for slot in range(1, n):
        copy = push(
            got_stats.at[0], got_stats.at[slot], stat_send.at[slot], stat_recv.at[slot], "vocab", xor_of(me, slot, n)
        )
        copy.start()
        copies.append(copy)
    for copy in copies:
        copy.wait()
    top = got_stats[0, :n]
    for slot in range(1, n):
        top = jnp.maximum(top, got_stats[slot, :n])
    total = jnp.zeros((n, tokens), f32)
    pick = jnp.zeros((n, tokens), f32)
    for slot in range(n):
        total = total + got_stats[slot, n : 2 * n] * jnp.exp(got_stats[slot, :n] - top)
        pick = pick + got_stats[slot, 2 * n : 3 * n]
    row_lse = top + jnp.log(total)
    weights = weights_ref[...]
    mine = lax.broadcasted_iota(jnp.int32, (n, tokens), 0) == me
    loss_row = jnp.sum(jnp.where(mine, weights * (row_lse - pick), 0.0), axis=0, keepdims=True)
    loss_lanes = loss_row[:, :128]
    for q in range(128, tokens, 128):
        loss_lanes = loss_lanes + loss_row[:, q : q + 128]
    loss_out[...] = jnp.broadcast_to(loss_lanes, loss_out.shape)
    spare = 128 - 2 * n
    lse_cols[...] = jnp.concatenate([row_lse, weights, jnp.zeros((spare, tokens), f32)], axis=0).T

    def scale_block(slot, out):
        block = xor_of(me, slot, n)
        goal_all = jnp.broadcast_to(column_of(columns[...], block), (tokens, 128))
        lse_all = jnp.broadcast_to(column_of(lse_cols[...], block), (tokens, 128))
        weight_all = jnp.broadcast_to(column_of(lse_cols[...], block + n), (tokens, 128))
        for first in range(0, tokens, step_rows):
            part = slice(first, first + step_rows)
            goal, weight, lse = goal_all[part], weight_all[part], lse_all[part]
            for index in range(chunks):
                factor = weight * jnp.exp(tops[slot, index, part] - lse)
                for q in range(index * chunk, (index + 1) * chunk, 128):
                    hit = jnp.where(small_lane + float(q) == goal, weight, 0.0)
                    grown = probs[slot, part, q : q + 128].astype(f32)
                    out[part, q : q + 128] = (grown * factor - hit).astype(bf16)

    def sib_copy(pair):
        return push(
            sib_send.at[lax.rem(pair, 2)],
            hid_all.at[2 * pair],
            sib_sem.at[pair],
            sib_recv.at[pair],
            "vocab",
            sibling,
        )

    def off_copy(pair):
        return push(
            off_send.at[lax.rem(pair, ring)],
            hid_all.at[2 * pair + 1],
            off_sem.at[pair],
            off_recv.at[pair],
            "vocab",
            xor_of(me, 2 * pair, n),
        )

    scale_block(n - 1, dl_a)

    def second_pass(trip, _):
        pair = pairs - 1 - trip

        @pl.when(trip > 1)
        def _():
            sib_copy(pair + 2).wait_send()

        scale_block(2 * pair, dl_b)
        sib_send[lax.rem(pair, 2)] = jnp.dot(dl_a[...], table[...], preferred_element_type=f32).astype(bf16)
        sib_copy(pair).start()

        scale_block(jnp.maximum(2 * pair - 1, 0), dl_a)
        partial[...] = jnp.dot(dl_b[...], table[...], preferred_element_type=f32)
        sib_copy(pair).wait_recv()

        @pl.when(pair > 0)
        def _():
            @pl.when(trip >= ring)
            def _():
                off_copy(pair + ring).wait_send()

            off_send[lax.rem(pair, ring)] = (partial[...] + hid_all[2 * pair].astype(f32)).astype(bf16)
            off_copy(pair).start()

        return 0

    lax.fori_loop(0, pairs, second_pass, 0)
    for pair in range(min(2, pairs)):
        sib_copy(pair).wait_send()
    for pair in range(1, pairs):
        if pair <= ring:
            off_copy(pair).wait_send()
        off_copy(pair).wait_recv()
    total = partial[...] + hid_all[0].astype(f32)
    for pair in range(1, pairs):
        total = total + hid_all[2 * pair + 1].astype(f32)
    dhid_out[...] = total


def head(n, hid, targets, weights, table):
    tokens, width = hid.shape
    rows = table.shape[0]
    padded = -(-rows // 128) * 128
    if rows % 16:
        table = jnp.pad(table, ((0, padded - rows), (0, 0)))
    groups = padded // 128
    per = max(part for part in range(1, 14) if groups % part == 0)
    chunk = per * 128
    f32, bf16 = jnp.float32, jnp.bfloat16
    dma = pltpu.SemaphoreType.DMA
    pairs = n // 2
    ring = max(1, min(pairs - 1, 3))
    return pl.pallas_call(
        functools.partial(head_kernel, n, rows, padded, chunk, VOCAB_REAL),
        out_shape=(jax.ShapeDtypeStruct((tokens, width), f32), jax.ShapeDtypeStruct((8, 128), f32)),
        in_specs=[vspec(), vspec(), vspec(), aspec()],
        out_specs=(vspec(), vspec()),
        scratch_shapes=[
            pltpu.VMEM((padded, width), bf16),
            pltpu.VMEM((n, tokens, padded), bf16),
            pltpu.VMEM((n, tokens, width), bf16),
            pltpu.VMEM((tokens, chunk), f32),
            pltpu.VMEM((tokens, chunk), f32),
            pltpu.VMEM((n, padded // chunk, tokens, 128), f32),
            pltpu.VMEM((tokens, 128), f32),
            pltpu.VMEM((tokens, 128), f32),
            pltpu.VMEM((tokens, 128), f32),
            pltpu.VMEM((tokens, 128), f32),
            pltpu.VMEM((tokens, 128), f32),
            pltpu.VMEM((n, 3 * n, tokens), f32),
            pltpu.VMEM((tokens, 128), f32),
            pltpu.VMEM((tokens, padded), bf16),
            pltpu.VMEM((tokens, padded), bf16),
            pltpu.VMEM((tokens, width), f32),
            pltpu.VMEM((2, tokens, width), bf16),
            pltpu.VMEM((ring, tokens, width), bf16),
            dma, dma, dma((n,)), dma((n,)), dma((n,)), dma((n,)), dma((n,)),
            dma((pairs,)), dma((pairs,)), dma((pairs,)), dma((pairs,)),
        ],
        compiler_params=pltpu.CompilerParams(
            collective_id=3, has_side_effects=True, vmem_limit_bytes=VMEM_CAP
        ),
        name="head",
    )(hid, targets, weights, table)


def local(
    token_ids,
    target_ids,
    loss_mask,
    seq_ids,
    embed_table,
    pos_table,
    gains,
    shifts,
    linear_bias,
    query_key_value_weight,
    w_out,
    w_fc,
    w_proj,
    adapters,
    first_moment,
    second_moment,
    step_count,
):
    vocab_place = lax.axis_index("vocab")
    vocab_count = lax.axis_size("vocab")
    total_tokens = TOK_DEV * vocab_count * lax.axis_size("dp")
    shard_rows = embed_table.shape[0]
    zero_row = jnp.zeros_like(token_ids)
    ints, adapter_parts = gather_meta(
        vocab_count,
        jnp.stack([token_ids, target_ids, loss_mask] + [zero_row] * 5),
        adapters.astype(jnp.bfloat16).reshape(-1, 128),
    )
    all_tokens = ints[:, 0].reshape(-1)
    copies = adapter_parts.reshape(1, -1)
    wanted = all_tokens - vocab_place * shard_rows
    inside = (wanted >= 0) & (wanted < shard_rows)
    picked_rows = jnp.take(embed_table, jnp.clip(wanted, 0, shard_rows - 1), axis=0)
    embedded = lax.psum_scatter(
        jnp.where(inside[:, None], picked_rows.astype(jnp.float32), 0.0).astype(jnp.bfloat16),
        "vocab",
        scatter_dimension=0,
        tiled=True,
    ).astype(jnp.float32)
    resid = embedded + pos_table[positions_of(seq_ids)].astype(jnp.float32)
    place = jnp.arange(TOK_DEV)
    visible = (seq_ids[:, None] == seq_ids[None, :]) & (place[None, :] <= place[:, None])
    layer_params = 0
    qkv_down_matrix, output_down_matrix, qkv_up_matrix, output_up_matrix = split_adapter(
        copies[layer_params]
    )
    bias_vector = linear_bias[layer_params]
    hidden_first, normed_one, inverse_one = layer_norm(
        resid, gains[2 * layer_params], shifts[2 * layer_params]
    )
    hidden_first = hidden_first.astype(jnp.bfloat16)
    adapter_input = mixed_product(hidden_first, qkv_down_matrix).astype(jnp.bfloat16)
    query_key_value = (
        mixed_product(hidden_first, query_key_value_weight[layer_params])
        + bias_vector[: 3 * MODEL_WIDTH]
        + ADAPTER_SCALE * mixed_product(adapter_input, qkv_up_matrix)
    )
    query_key_value = query_key_value.astype(jnp.bfloat16)
    attention_output, row_lse = attention_forward(query_key_value, visible)
    attention_output = attention_output.astype(jnp.bfloat16)
    adapter_middle = mixed_product(attention_output, output_down_matrix).astype(jnp.bfloat16)
    resid = (
        resid
        + mixed_product(attention_output, w_out[layer_params])
        + bias_vector[3 * MODEL_WIDTH : 4 * MODEL_WIDTH]
        + ADAPTER_SCALE * mixed_product(adapter_middle, output_up_matrix)
    )
    h_two, normed_two, inverse_two = layer_norm(
        resid, gains[2 * layer_params + 1], shifts[2 * layer_params + 1]
    )
    h_two = h_two.astype(jnp.bfloat16)
    pre = (
        mixed_product(h_two, w_fc[layer_params])
        + bias_vector[4 * MODEL_WIDTH : 4 * MODEL_WIDTH + FF]
    )
    act = gelu(pre).astype(jnp.bfloat16)
    resid = resid + mixed_product(act, w_proj[layer_params]) + bias_vector[4 * MODEL_WIDTH + FF :]
    saved = [
        (
            hidden_first,
            normed_one,
            inverse_one,
            adapter_input,
            query_key_value,
            row_lse,
            attention_output,
            adapter_middle,
            normed_two,
            inverse_two,
            pre,
        )
    ]
    hidden, normed_last, inverse_last = layer_norm(resid, gains[2 * LAYERS], shifts[2 * LAYERS])
    hidden = hidden.astype(jnp.bfloat16)
    grad_hidden, loss_rows = head(
        vocab_count,
        hidden,
        ints[:, 1].astype(jnp.float32),
        ints[:, 2].astype(jnp.float32) * (1.0 / total_tokens),
        embed_table,
    )
    grad_resid = norm_back(grad_hidden, normed_last, inverse_last, gains[2 * LAYERS])
    layer_grads = []
    for layer_params in reversed(range(LAYERS)):
        (
            hidden_first,
            normed_one,
            inverse_one,
            adapter_input,
            query_key_value,
            row_lse_l,
            attention_output,
            adapter_middle,
            normed_two,
            inverse_two,
            pre,
        ) = saved[layer_params]
        qkv_down_matrix, output_down_matrix, qkv_up_matrix, output_up_matrix = split_adapter(
            copies[layer_params]
        )
        grad_top = grad_resid.astype(jnp.bfloat16)
        grad_act = jnp.einsum(
            "te,fe->tf", grad_top, w_proj[layer_params], preferred_element_type=jnp.float32
        )
        grad_pre = jax.vjp(gelu, pre)[1](grad_act)[0].astype(jnp.bfloat16)
        grad_h_two = jnp.einsum(
            "tf,df->td", grad_pre, w_fc[layer_params], preferred_element_type=jnp.float32
        )
        grad_resid = grad_resid + norm_back(
            grad_h_two, normed_two, inverse_two, gains[2 * layer_params + 1]
        )
        middle_gradient = grad_resid.astype(jnp.bfloat16)
        adapter_middle_gradient = ADAPTER_SCALE * jnp.einsum(
            "te,re->tr", middle_gradient, output_up_matrix, preferred_element_type=jnp.float32
        )
        output_up_gradient = ADAPTER_SCALE * jnp.einsum(
            "iz,iq->zq", adapter_middle, middle_gradient, preferred_element_type=jnp.float32
        )
        output_down_gradient = exact_product(attention_output.T, adapter_middle_gradient)
        attention_output_gradient = jnp.einsum(
            "te,de->td", middle_gradient, w_out[layer_params], preferred_element_type=jnp.float32
        )
        attention_output_gradient = (
            attention_output_gradient + exact_product(adapter_middle_gradient, output_down_matrix.T)
        ).astype(jnp.bfloat16)
        query_key_value_gradient = attention_back(
            query_key_value, visible, row_lse_l, attention_output_gradient
        )
        qkv_up_gradient = ADAPTER_SCALE * jnp.einsum(
            "iz,iq->zq", adapter_input, query_key_value_gradient, preferred_element_type=jnp.float32
        )
        adapter_input_gradient = ADAPTER_SCALE * jnp.einsum(
            "te,re->tr", query_key_value_gradient, qkv_up_matrix, preferred_element_type=jnp.float32
        )
        qkv_down_gradient = exact_product(hidden_first.T, adapter_input_gradient)
        layer_grads.insert(
            0,
            jnp.concatenate(
                [
                    qkv_down_gradient.reshape(-1),
                    output_down_gradient.reshape(-1),
                    qkv_up_gradient.reshape(-1),
                    output_up_gradient.reshape(-1),
                ]
            ),
        )
    flat = layer_grads[0].reshape(vocab_count, -1, 128)
    shard_lines = flat.shape[1]
    spare = -(shard_lines + 1) % 8
    loss_line = jnp.broadcast_to(loss_rows[:1][None], (vocab_count, 1, 128))
    grads = jnp.concatenate(
        [flat, loss_line, jnp.zeros((vocab_count, spare, 128), jnp.float32)], axis=1
    )
    loss, grad_norm, new_adapters, new_first, new_second, rounded = finish(
        vocab_count,
        lax.axis_size("dp"),
        1.0,
        grads,
        adapters.reshape(-1, 128),
        first_moment.reshape(-1, 128),
        second_moment.reshape(-1, 128),
        step_count,
    )
    return (
        loss[0, 0],
        grad_norm[0, 0],
        new_adapters.reshape(1, -1),
        new_first.reshape(1, -1),
        new_second.reshape(1, -1),
        rounded.reshape(1, -1),
    )


def solution(mesh):
    in_specs = (
        P(("vocab", "dp")),
        P(("vocab", "dp")),
        P(("vocab", "dp")),
        P(("vocab", "dp")),
        P("vocab", None),
        P(),
        P(),
        P(),
        P(),
        P(),
        P(),
        P(),
        P(),
        P(None, "vocab"),
        P(None, "vocab"),
        P(None, "vocab"),
        P(),
    )
    out_specs = (P(), P(), P(None, "vocab"), P(None, "vocab"), P(None, "vocab"), P(None, "vocab"))
    return jax.shard_map(local, mesh=mesh, in_specs=in_specs, out_specs=out_specs, check_vma=False)
```
